16 devices in a mesh: dp: 2 (over z), pp: 8 (over y, x, core).
Axes of the slice: x: 2, y: 2, z: 2, core: 2. Of those that a mesh axis runs over, the one named last changes fastest.
Arguments:
- x: bfloat16 [8, 1024, 768], P(None, 'dp')
- t: bfloat16 [8, 1024, 768], P(None, 'dp')
- w1: bfloat16 [8, 2, 768, 3072], P('pp')
- w2: bfloat16 [8, 2, 3072, 768], P('pp')
Outputs:
- output 1: float32 [8, 2, 768, 3072], P('pp')
- output 2: float32 [8, 2, 3072, 768], P('pp')
- output 3: float32 [], replicated
All inputs are finite; a program needn't handle non-finite values.
Results may differ from the reference program's by a relative error of at most 0.00419436.
Values are sent between devices in bfloat16 or wider.
A program may use at most 1 GiB of HBM per device.

```python
import math
import jax
import jax.numpy as jnp
from jax import lax

D = 768
FF = 3072
STAGES = 8
MICRO = 8
TOKENS = 1024


def _gelu(u):
    c = math.sqrt(2.0 / math.pi)
    return 0.5 * u * (1.0 + jnp.tanh(c * (u + 0.044715 * u * u * u)))


def _dgelu(u):
    c = math.sqrt(2.0 / math.pi)
    th = jnp.tanh(c * (u + 0.044715 * u * u * u))
    return 0.5 * (1.0 + th) + 0.5 * u * (1.0 - th * th) * c * (1.0 + 3.0 * 0.044715 * u * u)


def setup_inputs(seed: int = 0) -> dict:
    k = jax.random.split(jax.random.PRNGKey(seed), 4)
    x = jax.random.normal(k[0], (MICRO, TOKENS, D), jnp.float32)
    t = jax.random.normal(k[1], (MICRO, TOKENS, D), jnp.float32)
    w1 = jax.random.normal(k[2], (STAGES, 2, D, FF), jnp.float32) * D ** -0.5
    w2 = jax.random.normal(k[3], (STAGES, 2, FF, D), jnp.float32) * (FF * STAGES) ** -0.5
    return {'x': x.astype(jnp.bfloat16), 't': t.astype(jnp.bfloat16),
            'w1': w1.astype(jnp.bfloat16), 'w2': w2.astype(jnp.bfloat16)}


def reference(x, t, w1, w2):
    nl = STAGES * 2
    w1f = w1.reshape(nl, D, FF)
    w2f = w2.reshape(nl, FF, D)
    inv = 1.0 / (MICRO * TOKENS * D)

    def fwd(h, w):
        a1, a2 = w
        u = jnp.dot(h, a1, preferred_element_type=jnp.float32).astype(jnp.bfloat16)
        a = _gelu(u.astype(jnp.float32)).astype(jnp.bfloat16)
        h2 = (h.astype(jnp.float32) + jnp.dot(a, a2, preferred_element_type=jnp.float32)).astype(jnp.bfloat16)
        return h2, (h, u)

    def bwd(g, z):
        h, u, a1, a2 = z
        uf = u.astype(jnp.float32)
        a = _gelu(uf).astype(jnp.bfloat16)
        q = jnp.dot(g, a2.T, preferred_element_type=jnp.float32)
        e = (_dgelu(uf) * q).astype(jnp.bfloat16)
        d2 = jnp.dot(a.T, g, preferred_element_type=jnp.float32)
        d1 = jnp.dot(h.T, e, preferred_element_type=jnp.float32)
        g2 = (g.astype(jnp.float32) + jnp.dot(e, a1.T, preferred_element_type=jnp.float32)).astype(jnp.bfloat16)
        return g2, (d1, d2)

    def micro(carry, xt):
        dw1, dw2, loss = carry
        xm, tm = xt
        y, (hs, us) = lax.scan(fwd, xm, (w1f, w2f))
        r = y.astype(jnp.float32) - tm.astype(jnp.float32)
        loss = loss + 0.5 * jnp.sum(r * r) * inv
        g = (r * inv).astype(jnp.bfloat16)
        _, (d1, d2) = lax.scan(bwd, g, (hs, us, w1f, w2f), reverse=True)
        return (dw1 + d1, dw2 + d2, loss), None

    init = (jnp.zeros((nl, D, FF), jnp.float32), jnp.zeros((nl, FF, D), jnp.float32),
            jnp.zeros((), jnp.float32))
    (dw1, dw2, loss), _ = lax.scan(micro, init, (x, t))
    return dw1.reshape(STAGES, 2, D, FF), dw2.reshape(STAGES, 2, FF, D), loss
```

```python
import functools
import math

import jax
import jax.numpy as jnp
from jax import lax
from jax.experimental import pallas as pl
from jax.experimental.pallas import tpu as pltpu
from jax.sharding import PartitionSpec as P

MESH = pl.DeviceIdType.MESH
BF, F32 = jnp.bfloat16, jnp.float32
ANY = pl.BlockSpec(memory_space=pl.ANY)
C0 = math.sqrt(2.0 / math.pi)
C1 = C0 * 0.044715
T = 256
CH = 768


def _nn(a, b):
    return jnp.dot(a, b, preferred_element_type=F32)


def _nt(a, b):
    return lax.dot_general(a, b, (((1,), (1,)), ((), ())), preferred_element_type=F32)


def _tn(a, b):
    return lax.dot_general(a, b, (((0,), (0,)), ((), ())), preferred_element_type=F32)


def _layer(x, n, first, point, second):
    r = x.astype(F32)
    q = first(x, 0)
    for c in range(n):
        ahead = first(x, c + 1) if c + 1 < n else None
        a = point(q, c)
        if second is not None:
            r = r + second(a, c)
        q = ahead
    return None if second is None else r.astype(BF)


def _stage_kernel(ndp, npp, nb, inv, x_ref, t_ref, w1_ref, w2_ref,
                  h_out, g_out, a_out, e_out, loss_out,
                  w1, w2, hin, gin, us, as_, ub, es, h1s, g0s, hst, gst, acc,
                  wsem, hrecv, grecv, xhrecv, xgrecv, zhsend, zgsend, hcp, gcp, h1sem, g0sem,
                  ussem, assem, ubsem, essem, hsend, gsend, lsend, lrecv):
    z = lax.axis_index("dp")
    s = lax.axis_index("pp")
    peer = (1 - z, s)
    ff = w1.shape[-1]
    nc = ff // CH
    first, last = s == 0, s == npp - 1

    loads = []
    for j in range(2):
        for k, (src, dst) in enumerate(((w1_ref, w1), (w2_ref, w2))):
            loads.append(pltpu.make_async_copy(src.at[j], dst.at[j], wsem.at[j, k]))
    for c in loads:
        c.start()

    barrier = pltpu.get_barrier_semaphore()
    for dz in range(ndp):
        for ds in range(npp):
            if dz or ds:
                pl.semaphore_signal(barrier, inc=1, device_id=((z + dz) % ndp, (s + ds) % npp), device_id_type=MESH)
    pl.semaphore_wait(barrier, ndp * npp - 1)

    def x_copy(m):
        return pltpu.make_async_copy(x_ref.at[m], hin.at[0, m], hrecv.at[m])

    def t_copy(m):
        return pltpu.make_async_copy(t_ref.at[m], gin.at[0, m], grecv.at[m])

    def each(n, f):
        def step(i, c):
            f(i)
            return c
        lax.fori_loop(0, n, step, 0)

    @pl.when(first)
    def _():
        each(nb, lambda m: x_copy(m).start())

    @pl.when(last)
    def _():
        each(nb, lambda m: t_copy(m).start())
        acc[...] = jnp.zeros_like(acc)

    def share(buf, m, send, recv):
        return pltpu.make_async_remote_copy(src_ref=buf.at[0, m], dst_ref=buf.at[1, m], send_sem=send.at[m], recv_sem=recv.at[m],
                                            device_id=peer, device_id_type=MESH)

    def pass_h(m, k):
        return pltpu.make_async_remote_copy(src_ref=hst.at[k], dst_ref=hin.at[0, m], send_sem=hsend.at[k], recv_sem=hrecv.at[m],
                                            device_id=(z, lax.rem(s + 1, npp)), device_id_type=MESH)

    def pass_g(m, k):
        return pltpu.make_async_remote_copy(src_ref=gst.at[k], dst_ref=gin.at[0, m], send_sem=gsend.at[k], recv_sem=grecv.at[m],
                                            device_id=(z, lax.rem(s + npp - 1, npp)), device_id_type=MESH)

    def u_out(j, r, m):
        return pltpu.make_async_copy(us.at[j], e_out.at[j, r, m], ussem.at[j])

    def a_outc(j, r, m):
        return pltpu.make_async_copy(as_.at[j], a_out.at[j, r, m], assem.at[j])

    def u_in(j, r, m):
        return pltpu.make_async_copy(e_out.at[j, r, m], ub.at[j], ubsem.at[j])

    def e_outc(j, r, m):
        return pltpu.make_async_copy(es.at[j], e_out.at[j, r, m], essem.at[j])

    def keep(src, dst, sem):
        return pltpu.make_async_copy(src, dst, sem)

    def gelu(j):
        def point(q, c):
            cs = pl.ds(c * CH, CH)
            u = q.astype(BF)
            us[j, :, cs] = u
            u = u.astype(F32)
            hu = 0.5 * u
            a = (hu + hu * jnp.tanh(u * (C0 + C1 * (u * u)))).astype(BF)
            as_[j, :, cs] = a
            return a
        return point

    def dgelu(j):
        def point(q, c):
            cs = pl.ds(c * CH, CH)
            u = ub[j, :, cs].astype(F32)
            u2 = u * u
            th = jnp.tanh(u * (C0 + C1 * u2))
            d = (0.5 + 0.5 * th) + (u * (0.5 * C0 + (1.5 * C1) * u2)) * (1.0 - th * th)
            e = (d * q).astype(BF)
            es[j, :, cs] = e
            return e
        return point

    def fwd(j, x, full=True):
        second = (lambda a, c: _nn(a, w2[j, pl.ds(c * CH, CH), :])) if full else None
        return _layer(x, nc, lambda x, c: _nn(x, w1[j, :, pl.ds(c * CH, CH)]), gelu(j), second)

    def bwd(j, g, full=True):
        second = (lambda e, c: _nt(e, w1[j, :, pl.ds(c * CH, CH)])) if full else None
        return _layer(g, nc, lambda g, c: _nt(g, w2[j, pl.ds(c * CH, CH), :]), dgelu(j), second)

    def drain_f():
        for j in range(2):
            u_out(j, 0, 0).wait()
            a_outc(j, 0, 0).wait()

    def fwd_task(o, m, idle):
        r = z if o == 0 else 1 - z
        if o == 0:
            x_copy(m).wait()
            share(hin, m, zhsend, xhrecv).start()
        else:
            share(hin, m, zhsend, xhrecv).wait_recv()
        keep(hin.at[o, m], h_out.at[0, r, m], hcp).start()

        @pl.when(jnp.logical_not(idle))
        def _():
            u_out(0, 0, 0).wait()
            a_outc(0, 0, 0).wait()

        if o == 0:
            @pl.when(m == 0)
            def _():
                loads[0].wait()
                loads[1].wait()

            @pl.when(m > 0)
            def _():
                keep(h1s, h_out.at[1, r, m], h1sem).wait()
        else:
            keep(h1s, h_out.at[1, r, m], h1sem).wait()
        h1s[...] = fwd(0, hin[o, m])
        u_out(0, r, m).start()
        a_outc(0, r, m).start()
        keep(h1s, h_out.at[1, r, m], h1sem).start()

        @pl.when(jnp.logical_not(idle))
        def _():
            u_out(1, 0, 0).wait()
            a_outc(1, 0, 0).wait()

        if o == 0:
            @pl.when(m == 0)
            def _():
                loads[2].wait()
                loads[3].wait()

            k = m % 2

            @pl.when(jnp.logical_and(m > 1, jnp.logical_not(last)))
            def _():
                pass_h(m, k).wait_send()
            hst[k] = fwd(1, h1s[...])
        else:
            fwd(1, h1s[...], full=False)
        u_out(1, r, m).start()
        a_outc(1, r, m).start()
        if o == 0:
            @pl.when(jnp.logical_not(last))
            def _():
                pass_h(m, k).start()

            @pl.when(last)
            def _():
                t_copy(m).wait()
                d = hst[k].astype(F32) - gin[0, m].astype(F32)
                gin[0, m] = (d * inv).astype(BF)
                p = jnp.sum((d * d).reshape(T // 8, 8, d.shape[-1]), axis=0)
                acc[...] += sum(p[:, i:i + 128] for i in range(0, d.shape[-1], 128))

    def bwd_task(o, m, b):
        r = z if o == 0 else 1 - z
        if o == 0:
            @pl.when(jnp.logical_not(last))
            def _():
                t_copy(m).wait()
            share(gin, m, zgsend, xgrecv).start()
        else:
            share(gin, m, zgsend, xgrecv).wait_recv()
        keep(gin.at[o, m], g_out.at[1, r, m], gcp).start()

        def ready(j):
            @pl.when(b > 0)
            def _():
                e_outc(j, 0, 0).wait()
                if j == 1:
                    keep(g0s, g_out.at[0, r, m], g0sem).wait()
            u_in(j, r, m).wait()

        def ahead(j):
            @pl.when(m + 1 < nb)
            def _():
                u_in(j, r, m + 1).start()

        ready(1)
        g0s[...] = bwd(1, gin[o, m])
        e_outc(1, r, m).start()
        keep(g0s, g_out.at[0, r, m], g0sem).start()
        ahead(1)
        ready(0)
        if o == 0:
            k = m % 2

            @pl.when(jnp.logical_and(m > 1, jnp.logical_not(first)))
            def _():
                pass_g(m, k).wait_send()
            gst[k] = bwd(0, g0s[...])
        else:
            bwd(0, g0s[...], full=False)
        e_outc(0, r, m).start()
        ahead(0)
        if o == 0:
            @pl.when(jnp.logical_not(first))
            def _():
                pass_g(m, k).start()

    room = jnp.minimum(nb, (8 * (npp - 1 - s)) // 3)

    def task(i, c):
        @pl.when(i < nb)
        def _():
            fwd_task(0, i, i == 0)

        early = jnp.logical_and(i >= nb, i < nb + room)
        late = jnp.logical_and(i >= 2 * nb + room, i < 3 * nb)

        @pl.when(jnp.logical_or(early, late))
        def _():
            m = jnp.where(early, i - nb, i - 2 * nb)
            fwd_task(1, m, m == 0)

        @pl.when(jnp.logical_and(i >= nb + room, i < 2 * nb + room))
        def _():
            m = i - nb - room
            bwd_task(0, m, m)

        @pl.when(i >= 3 * nb)
        def _():
            m = i - 3 * nb
            bwd_task(1, m, m + nb)

        for end, r in ((nb - 1, z), (3 * nb - 1, 1 - z)):
            @pl.when(i == end)
            def _():
                drain_f()
                for j in (1, 0):
                    u_in(j, r, 0).start()
        return c

    lax.fori_loop(0, 4 * nb, task, 0)

    def loss_copy(dz, ds):
        return pltpu.make_async_remote_copy(src_ref=acc, dst_ref=loss_out.at[z], send_sem=lsend.at[dz * npp + ds],
                                            recv_sem=lrecv.at[z],
                                            device_id=((z + dz) % ndp, (s + ds) % npp), device_id_type=MESH)

    def loss_own():
        return pltpu.make_async_copy(acc, loss_out.at[z], lrecv.at[z])

    @pl.when(last)
    def _():
        loss_own().start()
        for dz in range(ndp):
            for ds in range(npp):
                if dz or ds:
                    loss_copy(dz, ds).start()
        for dz in range(ndp):
            for ds in range(npp):
                if dz or ds:
                    loss_copy(dz, ds).wait_send()
    for d in range(ndp):
        pltpu.make_async_copy(acc, loss_out.at[d], lrecv.at[d]).wait()

    def sent(m):
        share(hin, m, zhsend, xhrecv).wait_send()
        share(gin, m, zgsend, xgrecv).wait_send()
    each(nb, sent)
    for k in range(2):
        @pl.when(jnp.logical_not(last))
        def _():
            pass_h(0, k).wait_send()

        @pl.when(jnp.logical_not(first))
        def _():
            pass_g(0, k).wait_send()
    keep(hin, h_out.at[0], hcp).wait()
    keep(gin, g_out.at[1], gcp).wait()
    keep(h1s, h_out.at[1, 0, 0], h1sem).wait()
    keep(g0s, g_out.at[0, 0, 0], g0sem).wait()
    for j in range(2):
        e_outc(j, 0, 0).wait()


def _stages(x, t, w1, w2, ndp, npp, inv):
    nb, _, d = x.shape
    ff = w1.shape[-1]
    dma = pltpu.SemaphoreType.DMA
    act = jax.ShapeDtypeStruct((2, ndp, nb, T, d), BF)
    wide = jax.ShapeDtypeStruct((2, ndp, nb, T, ff), BF)
    flops = 28 * nb * T * d * ff
    return pl.pallas_call(
        functools.partial(_stage_kernel, ndp, npp, nb, inv),
        out_shape=(act, act, wide, wide, jax.ShapeDtypeStruct((ndp, 8, 128), F32)),
        in_specs=[ANY] * 4,
        out_specs=(ANY,) * 5,
        scratch_shapes=[
            pltpu.VMEM((2, d, ff), BF), pltpu.VMEM((2, ff, d), BF),
            pltpu.VMEM((ndp, nb, T, d), BF), pltpu.VMEM((ndp, nb, T, d), BF),
            pltpu.VMEM((2, T, ff), BF), pltpu.VMEM((2, T, ff), BF), pltpu.VMEM((2, T, ff), BF), pltpu.VMEM((2, T, ff), BF),
            pltpu.VMEM((T, d), BF), pltpu.VMEM((T, d), BF), pltpu.VMEM((2, T, d), BF), pltpu.VMEM((2, T, d), BF),
            pltpu.VMEM((8, 128), F32),
            dma((2, 2)), dma((nb,)), dma((nb,)), dma((nb,)), dma((nb,)), dma((nb,)), dma((nb,)), dma, dma, dma, dma,
            dma((2,)), dma((2,)), dma((2,)), dma((2,)), dma((2,)), dma((2,)), dma((ndp * npp,)), dma((ndp,)),
        ],
        compiler_params=pltpu.CompilerParams(collective_id=0, has_side_effects=True, vmem_limit_bytes=67_043_328),
        cost_estimate=pl.CostEstimate(flops=flops, bytes_accessed=16 * nb * T * ff, transcendentals=8 * nb * T * ff),
        name="stage",
    )(x, t, w1, w2)


def _dw_kernel(a_ref, b_ref, o_ref):
    o_ref[...] = _tn(a_ref[...], b_ref[...])


def _dw(a, b, wide_left):
    n, tokens, p = a.shape
    q = b.shape[-1]
    tile = 512
    whole = lambda w: pl.BlockSpec((None, tokens, w), lambda j, i: (j, 0, 0))
    part = pl.BlockSpec((None, tokens, tile), lambda j, i: (j, 0, i))
    if wide_left:
        grid, specs, out = (n, p // tile), [part, whole(q)], pl.BlockSpec((None, tile, q), lambda j, i: (j, i, 0))
    else:
        grid, specs, out = (n, q // tile), [whole(p), part], pl.BlockSpec((None, p, tile), lambda j, i: (j, 0, i))
    return pl.pallas_call(
        _dw_kernel,
        grid=grid,
        out_shape=jax.ShapeDtypeStruct((n, p, q), F32),
        in_specs=specs,
        out_specs=out,
        compiler_params=pltpu.CompilerParams(vmem_limit_bytes=62 * 1024 * 1024),
        cost_estimate=pl.CostEstimate(flops=2 * n * tokens * p * q, bytes_accessed=4 * n * tokens * q, transcendentals=0),
    )(a, b)


def solution(mesh):
    ndp = mesh.shape["dp"]
    npp = mesh.shape["pp"]

    def body(x, t, w1, w2):
        nm, tok, d = x.shape
        ff = w1.shape[-1]
        inv = 1.0 / (nm * tok * ndp * d)
        nb = nm * tok // T
        h, g, a, e, loss = _stages(x.reshape(nb, T, d), t.reshape(nb, T, d), w1[0], w2[0], ndp, npp, inv)
        n = ndp * nb * T
        dw1 = _dw(h.reshape(2, n, d), e.reshape(2, n, ff), False)
        dw2 = _dw(a.reshape(2, n, ff), g.reshape(2, n, d), True)
        return dw1[None], dw2[None], 0.5 * inv * jnp.sum(loss)

    return jax.shard_map(body, mesh=mesh,
                         in_specs=(P(None, 'dp', None), P(None, 'dp', None), P('pp'), P('pp')),
                         out_specs=(P('pp'), P('pp'), P()), check_vma=False)
```

```python
import functools
import math

import jax
import jax.numpy as jnp
from jax import lax
from jax.experimental import pallas as pl
from jax.experimental.pallas import tpu as pltpu
from jax.sharding import PartitionSpec as P

MESH = pl.DeviceIdType.MESH
BF, F32 = jnp.bfloat16, jnp.float32
ANY = pl.BlockSpec(memory_space=pl.ANY)
C0 = math.sqrt(2.0 / math.pi)
C1 = C0 * 0.044715
T = 256
TF = 128
CH = 768


def _nn(a, b):
    return jnp.dot(a, b, preferred_element_type=F32)


def _nt(a, b):
    return lax.dot_general(a, b, (((1,), (1,)), ((), ())), preferred_element_type=F32)


def _tn(a, b):
    return lax.dot_general(a, b, (((0,), (0,)), ((), ())), preferred_element_type=F32)


def _layer(x, n, first, point, second):
    r = x.astype(F32)
    q = first(x, 0)
    for c in range(n):
        ahead = first(x, c + 1) if c + 1 < n else None
        a = point(q, c)
        if second is not None:
            r = r + second(a, c)
        q = ahead
    return None if second is None else r.astype(BF)


def _stage_kernel(ndp, npp, nb, inv, x_ref, t_ref, w1_ref, w2_ref,
                  h_out, g_out, a_out, e_out, loss_out,
                  w1, w2, hin, gin, us, as_, ub, es, h1s, g0s, hst, gst, acc,
                  wsem, hrecv, grecv, xhrecv, xgrecv, zhsend, zgsend, hcp, gcp, h1sem, g0sem,
                  ussem, assem, ubsem, essem, hsend, gsend, lsend, lrecv):
    z = lax.axis_index("dp")
    s = lax.axis_index("pp")
    peer = (1 - z, s)
    ff = w1.shape[-1]
    nc = ff // CH
    first, last = s == 0, s == npp - 1

    loads = []
    for j in range(2):
        for k, (src, dst) in enumerate(((w1_ref, w1), (w2_ref, w2))):
            loads.append(pltpu.make_async_copy(src.at[j], dst.at[j], wsem.at[j, k]))
    for c in loads:
        c.start()

    barrier = pltpu.get_barrier_semaphore()
    for dz in range(ndp):
        for ds in range(npp):
            if dz or ds:
                pl.semaphore_signal(barrier, inc=1, device_id=((z + dz) % ndp, (s + ds) % npp), device_id_type=MESH)
    pl.semaphore_wait(barrier, ndp * npp - 1)

    per = T // TF

    def part(i):
        return lax.div(i, per), pl.ds(pl.multiple_of(lax.rem(i, per) * TF, TF), TF)

    def x_copy(i):
        return pltpu.make_async_copy(x_ref.at[part(i)], hin.at[0, *part(i)], hrecv.at[i])

    def t_copy(m):
        return pltpu.make_async_copy(t_ref.at[m], gin.at[0, m], grecv.at[m])

    def each(n, f):
        def step(i, c):
            f(i)
            return c
        lax.fori_loop(0, n, step, 0)

    @pl.when(first)
    def _():
        each(per * nb, lambda i: x_copy(i).start())

    @pl.when(last)
    def _():
        each(nb, lambda m: t_copy(m).start())
        acc[...] = jnp.zeros_like(acc)

    def share_h(i):
        return pltpu.make_async_remote_copy(src_ref=hin.at[0, *part(i)], dst_ref=hin.at[1, *part(i)], send_sem=zhsend.at[i],
                                            recv_sem=xhrecv.at[i], device_id=peer, device_id_type=MESH)

    def share_g(m):
        return pltpu.make_async_remote_copy(src_ref=gin.at[0, m], dst_ref=gin.at[1, m], send_sem=zgsend.at[m],
                                            recv_sem=xgrecv.at[m], device_id=peer, device_id_type=MESH)

    def pass_h(i, k):
        return pltpu.make_async_remote_copy(src_ref=hst.at[k], dst_ref=hin.at[0, *part(i)], send_sem=hsend.at[k],
                                            recv_sem=hrecv.at[i], device_id=(z, lax.rem(s + 1, npp)), device_id_type=MESH)

    def pass_g(m, k):
        return pltpu.make_async_remote_copy(src_ref=gst.at[k], dst_ref=gin.at[0, m], send_sem=gsend.at[k], recv_sem=grecv.at[m],
                                            device_id=(z, lax.rem(s + npp - 1, npp)), device_id_type=MESH)

    def f_out(j, r, m):
        return (pltpu.make_async_copy(us.at[j], e_out.at[j, r, m], ussem.at[j, 0]),
                pltpu.make_async_copy(as_.at[j], a_out.at[j, r, m], assem.at[j, 0]))

    def f_out_part(j, i, k):
        m, rows = part(i)
        mine = pl.ds(pl.multiple_of(k * TF, TF), TF)
        return (pltpu.make_async_copy(us.at[j, mine], e_out.at[j, z, m, rows], ussem.at[j, k]),
                pltpu.make_async_copy(as_.at[j, mine], a_out.at[j, z, m, rows], assem.at[j, k]))

    def u_in(j, r, m):
        return pltpu.make_async_copy(e_out.at[j, r, m], ub.at[j], ubsem.at[j])

    def e_outc(j, r, m):
        return pltpu.make_async_copy(es.at[j], e_out.at[j, r, m], essem.at[j])

    def keep(src, dst, sem):
        return pltpu.make_async_copy(src, dst, sem)

    def gelu(j, rows):
        def point(q, c):
            cs = pl.ds(c * CH, CH)
            u = q.astype(BF)
            us[j, rows, cs] = u
            u = u.astype(F32)
            a = ((0.5 * u) * (1.0 + jnp.tanh(u * (C0 + C1 * (u * u))))).astype(BF)
            as_[j, rows, cs] = a
            return a
        return point

    def dgelu(j):
        def point(q, c):
            cs = pl.ds(c * CH, CH)
            u = jnp.clip(ub[j, :, cs], -30.0, 30.0).astype(F32)
            k = C1 * (u * u)
            th = jnp.tanh(u * (C0 + k))
            d = (1.0 + th) * (0.5 + (1.0 - th) * (u * (0.5 * C0 + 1.5 * k)))
            e = (d * q).astype(BF)
            es[j, :, cs] = e
            return e
        return point

    def fwd(j, x, rows, full=True):
        second = (lambda a, c: _nn(a, w2[j, pl.ds(c * CH, CH), :])) if full else None
        return _layer(x, nc, lambda x, c: _nn(x, w1[j, :, pl.ds(c * CH, CH)]), gelu(j, rows), second)

    def bwd(j, g, full=True):
        second = (lambda e, c: _nt(e, w1[j, :, pl.ds(c * CH, CH)])) if full else None
        return _layer(g, nc, lambda g, c: _nt(g, w2[j, pl.ds(c * CH, CH), :]), dgelu(j), second)

    def start(copies):
        for c in copies:
            c.start()

    def wait(copies):
        for c in copies:
            c.wait()

    def fwd_own(i):
        m, rows = part(i)
        k = lax.rem(i, 2)
        mine = pl.ds(pl.multiple_of(k * TF, TF), TF)
        x_copy(i).wait()
        share_h(i).start()
        keep(hin.at[0, m, rows], h_out.at[0, z, m, rows], hcp).start()

        @pl.when(i == 0)
        def _():
            wait(loads[:2])

        def h1_out():
            return keep(h1s.at[mine], h_out.at[1, z, m, rows], h1sem.at[k])

        @pl.when(i > 1)
        def _():
            wait(f_out_part(0, i, k))
            h1_out().wait()
        h1s[mine] = fwd(0, hin[0, m, rows], mine)
        start(f_out_part(0, i, k))
        h1_out().start()

        @pl.when(i == 0)
        def _():
            wait(loads[2:])

        @pl.when(i > 1)
        def _():
            wait(f_out_part(1, i, k))

            @pl.when(jnp.logical_not(last))
            def _():
                pass_h(i, k).wait_send()
        hst[k] = fwd(1, h1s[mine], mine)
        start(f_out_part(1, i, k))

        @pl.when(jnp.logical_not(last))
        def _():
            pass_h(i, k).start()

        @pl.when(last)
        def _():
            @pl.when(lax.rem(i, per) == 0)
            def _():
                t_copy(m).wait()
            d = hst[k].astype(F32) - gin[0, m, rows].astype(F32)
            gin[0, m, rows] = (d * inv).astype(BF)
            p = jnp.sum((d * d).reshape(TF // 8, 8, d.shape[-1]), axis=0)
            acc[...] += sum(p[:, c:c + 128] for c in range(0, d.shape[-1], 128))

    def fwd_other(m):
        r = 1 - z
        rows = pl.ds(0, T)
        for p in range(per):
            share_h(per * m + p).wait_recv()
        keep(hin.at[1, m], h_out.at[0, r, m], hcp).start()

        @pl.when(m > 0)
        def _():
            wait(f_out(0, r, m))
            keep(h1s, h_out.at[1, r, m], h1sem.at[0]).wait()
        h1s[...] = fwd(0, hin[1, m], rows)
        start(f_out(0, r, m))
        keep(h1s, h_out.at[1, r, m], h1sem.at[0]).start()

        @pl.when(m > 0)
        def _():
            wait(f_out(1, r, m))
        fwd(1, h1s[...], rows, full=False)
        start(f_out(1, r, m))

    def bwd_task(o, m, b):
        r = z if o == 0 else 1 - z
        if o == 0:
            @pl.when(jnp.logical_not(last))
            def _():
                t_copy(m).wait()
            share_g(m).start()
        else:
            share_g(m).wait_recv()
        keep(gin.at[o, m], g_out.at[1, r, m], gcp).start()

        def ready(j):
            @pl.when(b > 0)
            def _():
                e_outc(j, 0, 0).wait()
                if j == 1:
                    keep(g0s, g_out.at[0, r, m], g0sem).wait()
            u_in(j, r, m).wait()

        def ahead(j):
            @pl.when(m + 1 < nb)
            def _():
                u_in(j, r, m + 1).start()

        ready(1)
        g0s[...] = bwd(1, gin[o, m])
        e_outc(1, r, m).start()
        keep(g0s, g_out.at[0, r, m], g0sem).start()
        ahead(1)
        ready(0)
        if o == 0:
            k = m % 2

            @pl.when(jnp.logical_and(m > 1, jnp.logical_not(first)))
            def _():
                pass_g(m, k).wait_send()
            gst[k] = bwd(0, g0s[...])
        else:
            bwd(0, g0s[...], full=False)
        e_outc(0, r, m).start()
        ahead(0)
        if o == 0:
            @pl.when(jnp.logical_not(first))
            def _():
                pass_g(m, k).start()

    def loss_copy(dz, ds):
        return pltpu.make_async_remote_copy(src_ref=acc, dst_ref=loss_out.at[z], send_sem=lsend.at[dz * npp + ds],
                                            recv_sem=lrecv.at[z],
                                            device_id=((z + dz) % ndp, (s + ds) % npp), device_id_type=MESH)

    def loss_own():
        return pltpu.make_async_copy(acc, loss_out.at[z], lrecv.at[z])

    others = [(dz, ds) for dz in range(ndp) for ds in range(npp) if dz or ds]

    def send_loss():
        loss_own().start()
        for dz, ds in others:
            loss_copy(dz, ds).start()

    room = jnp.minimum(nb, (8 * (npp - 1 - s)) // 3)

    nf = per * nb
    a, b, c, d = nf + room, nf + room + nb, nf + 2 * nb, nf + 3 * nb

    def load_u(r):
        for j in (1, 0):
            u_in(j, r, 0).start()

    def task(i, carry):
        @pl.when(i < nf)
        def _():
            fwd_own(i)

        @pl.when(i == nf - 1)
        def _():
            for j in range(2):
                for k in range(2):
                    wait(f_out_part(j, 0, k))
            for k in range(2):
                keep(h1s.at[pl.ds(k * TF, TF)], h_out.at[1, z, 0, pl.ds(k * TF, TF)], h1sem.at[k]).wait()
            load_u(z)
            pl.when(last)(send_loss)

        early = jnp.logical_and(i >= nf, i < a)
        late = jnp.logical_and(i >= b, i < c)

        @pl.when(jnp.logical_or(early, late))
        def _():
            fwd_other(jnp.where(early, i - nf, i - nf - nb))

        @pl.when(jnp.logical_and(i >= a, i < b))
        def _():
            bwd_task(0, i - a, i - a)

        @pl.when(i == c - 1)
        def _():
            for j in range(2):
                wait(f_out(j, 0, 0))
            load_u(1 - z)

        @pl.when(i >= c)
        def _():
            bwd_task(1, i - c, i - c + nb)
        return carry

    lax.fori_loop(0, d, task, 0)

    @pl.when(last)
    def _():
        for dz, ds in others:
            loss_copy(dz, ds).wait_send()
    for d in range(ndp):
        pltpu.make_async_copy(acc, loss_out.at[d], lrecv.at[d]).wait()
    each(nf, lambda i: share_h(i).wait_send())
    each(nb, lambda m: share_g(m).wait_send())
    for k in range(2):
        @pl.when(jnp.logical_not(last))
        def _():
            pass_h(0, k).wait_send()

        @pl.when(jnp.logical_not(first))
        def _():
            pass_g(0, k).wait_send()
    keep(hin, h_out.at[0], hcp).wait()
    keep(gin, g_out.at[1], gcp).wait()
    keep(h1s, h_out.at[1, 0, 0], h1sem.at[0]).wait()
    keep(g0s, g_out.at[0, 0, 0], g0sem).wait()
    for j in range(2):
        e_outc(j, 0, 0).wait()


def _stages(x, t, w1, w2, ndp, npp, inv):
    nb, _, d = x.shape
    ff = w1.shape[-1]
    nf = nb * T // TF
    dma = pltpu.SemaphoreType.DMA
    act = jax.ShapeDtypeStruct((2, ndp, nb, T, d), BF)
    wide = jax.ShapeDtypeStruct((2, ndp, nb, T, ff), BF)
    flops = 28 * nb * T * d * ff
    return pl.pallas_call(
        functools.partial(_stage_kernel, ndp, npp, nb, inv),
        out_shape=(act, act, wide, wide, jax.ShapeDtypeStruct((ndp, 8, 128), F32)),
        in_specs=[ANY] * 4,
        out_specs=(ANY,) * 5,
        scratch_shapes=[
            pltpu.VMEM((2, d, ff), BF), pltpu.VMEM((2, ff, d), BF),
            pltpu.VMEM((ndp, nb, T, d), BF), pltpu.VMEM((ndp, nb, T, d), BF),
            pltpu.VMEM((2, T, ff), BF), pltpu.VMEM((2, T, ff), BF), pltpu.VMEM((2, T, ff), BF), pltpu.VMEM((2, T, ff), BF),
            pltpu.VMEM((T, d), BF), pltpu.VMEM((T, d), BF), pltpu.VMEM((2, TF, d), BF), pltpu.VMEM((2, T, d), BF),
            pltpu.VMEM((8, 128), F32),
            dma((2, 2)), dma((nf,)), dma((nb,)), dma((nf,)), dma((nb,)), dma((nf,)), dma((nb,)), dma, dma, dma((2,)), dma,
            dma((2, 2)), dma((2, 2)), dma((2,)), dma((2,)), dma((2,)), dma((2,)), dma((ndp * npp,)), dma((ndp,)),
        ],
        compiler_params=pltpu.CompilerParams(collective_id=0, has_side_effects=True, vmem_limit_bytes=67_043_328),
        cost_estimate=pl.CostEstimate(flops=flops, bytes_accessed=16 * nb * T * ff, transcendentals=8 * nb * T * ff),
        name="stage",
    )(x, t, w1, w2)


def _half_kernel(z_ref, h_ref, e_ref, o_ref):
    p = _tn(h_ref[...], e_ref[...])
    k = pl.program_id(0)

    @pl.when(k == 0)
    def _():
        o_ref[...] = p

    @pl.when(k > 0)
    def _():
        o_ref[...] += p


def _half(h, e, z):
    _, n, d = h.shape
    ff = e.shape[-1]
    step = 2048
    return pl.pallas_call(
        _half_kernel,
        grid_spec=pltpu.PrefetchScalarGridSpec(
            num_scalar_prefetch=1,
            grid=(n // step,),
            in_specs=[pl.BlockSpec((None, step, d), lambda k, z: (0, k, 0)),
                      pl.BlockSpec((None, step, ff // 2), lambda k, z: (0, k, z[0]))],
            out_specs=pl.BlockSpec((d, ff // 2), lambda k, z: (0, 0)),
        ),
        out_shape=jax.ShapeDtypeStruct((d, ff // 2), F32),
        compiler_params=pltpu.CompilerParams(vmem_limit_bytes=62 * 1024 * 1024),
        cost_estimate=pl.CostEstimate(flops=n * d * ff, bytes_accessed=n * (2 * d + ff), transcendentals=0),
        name="half",
    )(z, h, e)


def _dw_kernel(h_ref, e_ref, a_ref, g_ref, s_ref, o1_ref, o2_ref, res, tile, o1, o2, sv, rsem, tsem, osem, ssem, vsem):
    z = lax.axis_index("dp")
    ff = e_ref.shape[-1]
    w = tile.shape[-1]
    per = ff // w
    steps = 3 * per
    cols = lambda t: pl.ds(pl.multiple_of(t * w, w), w)

    def resident(p):
        slot = p % 2
        src = h_ref.at[1] if p == 0 else g_ref.at[p - 1]
        return pltpu.make_async_copy(src, res.at[slot], rsem.at[slot])

    def stream_e(i):
        return pltpu.make_async_copy(e_ref.at[1, :, cols(i)], tile.at[lax.rem(i, 2)], tsem.at[lax.rem(i, 2)])

    def stream_a(i):
        j = lax.div(i, per) - 1
        return pltpu.make_async_copy(a_ref.at[j, :, cols(i - per * (j + 1))], tile.at[lax.rem(i, 2)], tsem.at[lax.rem(i, 2)])

    def put1(i):
        return pltpu.make_async_copy(o1.at[lax.rem(i, 2)], o1_ref.at[1, :, cols(i)], osem.at[lax.rem(i, 2)])

    def put2(i):
        j = lax.div(i, per) - 1
        return pltpu.make_async_copy(o2.at[lax.rem(i, 2)], o2_ref.at[j, cols(i - per * (j + 1)), :], osem.at[lax.rem(i, 2)])

    halves = [(pltpu.make_async_copy(s_ref.at[:, pl.ds(t * w, w)], sv.at[t], ssem.at[t]),
               pltpu.make_async_copy(sv.at[t], o1_ref.at[0, :, cols(z * (per // 2) + t)], vsem.at[t])) for t in range(per // 2)]

    resident(0).start()
    stream_e(0).start()

    def step(i, carry):
        @pl.when(i + 1 < per)
        def _():
            stream_e(i + 1).start()

        @pl.when(jnp.logical_and(i + 1 >= per, i + 1 < steps))
        def _():
            stream_a(i + 1).start()

        for p in range(3):
            @pl.when(i == per * p)
            def _():
                resident(p).wait()

            if p < 2:
                @pl.when(i == per * p + 1)
                def _():
                    resident(p + 1).start()
        for t, (get, put) in enumerate(halves):
            @pl.when(i == 2 + 2 * t)
            def _():
                get.start()

            @pl.when(i == 3 + 2 * t)
            def _():
                get.wait()
                put.start()
        k = lax.rem(i, 2)
        pltpu.make_async_copy(e_ref.at[1, :, pl.ds(0, w)], tile.at[k], tsem.at[k]).wait()

        @pl.when(i > 1)
        def _():
            pltpu.make_async_copy(o1.at[k], o1_ref.at[1, :, pl.ds(0, w)], osem.at[k]).wait()
        r = lax.rem(lax.div(i, per), 2)

        @pl.when(i < per)
        def _():
            o1[k] = _tn(res[r], tile[k])
            put1(i).start()

        @pl.when(i >= per)
        def _():
            o2[k] = _tn(tile[k], res[r])
            put2(i).start()
        return carry

    lax.fori_loop(0, steps, step, 0)
    for i in (steps - 2, steps - 1):
        put2(jnp.int32(i)).wait()
    for _, put in halves:
        put.wait()


def _dw(h, e, a, g, half):
    n, d = h.shape[1:]
    ff = e.shape[-1]
    w = 512
    dma = pltpu.SemaphoreType.DMA
    return pl.pallas_call(
        _dw_kernel,
        out_shape=(jax.ShapeDtypeStruct((2, d, ff), F32), jax.ShapeDtypeStruct((2, ff, d), F32)),
        in_specs=[ANY] * 5,
        out_specs=(ANY, ANY),
        scratch_shapes=[
            pltpu.VMEM((2, n, d), BF), pltpu.VMEM((2, n, w), BF), pltpu.VMEM((2, d, w), F32), pltpu.VMEM((2, w, d), F32),
            pltpu.VMEM((ff // w // 2, d, w), F32),
            dma((2,)), dma((2,)), dma((2,)), dma((ff // w // 2,)), dma((ff // w // 2,)),
        ],
        compiler_params=pltpu.CompilerParams(vmem_limit_bytes=62 * 1024 * 1024),
        cost_estimate=pl.CostEstimate(flops=6 * n * d * ff, bytes_accessed=6 * n * ff, transcendentals=0),
        name="dw",
    )(h, e, a, g, half)


def solution(mesh):
    ndp = mesh.shape["dp"]
    npp = mesh.shape["pp"]

    def body(x, t, w1, w2):
        nm, tok, d = x.shape
        ff = w1.shape[-1]
        inv = 1.0 / (nm * tok * ndp * d)
        nb = nm * tok // T
        h, g, a, e, loss = _stages(x.reshape(nb, T, d), t.reshape(nb, T, d), w1[0], w2[0], ndp, npp, inv)
        n = ndp * nb * T
        h, g, a, e = (v.reshape(2, n, v.shape[-1]) for v in (h, g, a, e))
        z = lax.axis_index("dp")
        half = _half(h, e, jnp.full((1,), z, jnp.int32))
        other = lax.ppermute(half, "dp", [(i, (i + 1) % ndp) for i in range(ndp)])
        dw1, dw2 = _dw(h, e, a, g, half)
        dw1 = lax.dynamic_update_slice(dw1, other[None], (0, 0, (1 - z) * (ff // 2)))
        return dw1[None], dw2[None], 0.5 * inv * jnp.sum(loss)

    return jax.shard_map(body, mesh=mesh,
                         in_specs=(P(None, 'dp', None), P(None, 'dp', None), P('pp'), P('pp')),
                         out_specs=(P('pp'), P('pp'), P()), check_vma=False)
```

```python
import functools
import math

import jax
import jax.numpy as jnp
from jax import lax
from jax.experimental import pallas as pl
from jax.experimental.pallas import tpu as pltpu
from jax.sharding import PartitionSpec as P

MESH = pl.DeviceIdType.MESH
BF, F32 = jnp.bfloat16, jnp.float32
ANY = pl.BlockSpec(memory_space=pl.ANY)
C0 = math.sqrt(2.0 / math.pi)
C1 = C0 * 0.044715
T = 256
TF = 128
CH = 768


def _nn(a, b):
    return jnp.dot(a, b, preferred_element_type=F32)


def _nt(a, b):
    return lax.dot_general(a, b, (((1,), (1,)), ((), ())), preferred_element_type=F32)


def _tn(a, b):
    return lax.dot_general(a, b, (((0,), (0,)), ((), ())), preferred_element_type=F32)


def _layer(x, n, first, point, second):
    r = x.astype(F32)
    q = first(x, 0)
    for c in range(n):
        ahead = first(x, c + 1) if c + 1 < n else None
        a = point(q, c)
        if second is not None:
            r = r + second(a, c)
        q = ahead
    return None if second is None else r.astype(BF)


def _stage_kernel(ndp, npp, nb, inv, x_ref, t_ref, w1_ref, w2_ref,
                  h_out, g_out, a_out, e_out, loss_out,
                  w1, w2, hin, gin, us, as_, ub, es, h1s, g0s, hst, gst, acc,
                  wsem, hrecv, grecv, xhrecv, xgrecv, zhsend, zgsend, hcp, gcp, h1sem, g0sem,
                  ussem, assem, ubsem, essem, hsend, gsend, lsend, lrecv):
    z = lax.axis_index("dp")
    s = lax.axis_index("pp")
    peer = (1 - z, s)
    ff = w1.shape[-1]
    nc = ff // CH
    first, last = s == 0, s == npp - 1

    per = T // TF

    def part(i):
        return lax.div(i, per), pl.ds(pl.multiple_of(lax.rem(i, per) * TF, TF), TF)

    def x_copy(i):
        return pltpu.make_async_copy(x_ref.at[part(i)], hin.at[0, *part(i)], hrecv.at[i])

    def t_copy(m):
        return pltpu.make_async_copy(t_ref.at[m], gin.at[0, m], grecv.at[m])

    def each(n, f):
        def step(i, c):
            f(i)
            return c
        lax.fori_loop(0, n, step, 0)

    @pl.when(first)
    def _():
        x_copy(0).start()

    @pl.when(last)
    def _():
        each(nb, lambda m: t_copy(m).start())
        acc[...] = jnp.zeros_like(acc)

    loads = []
    for j in range(2):
        for k, (src, dst) in enumerate(((w1_ref, w1), (w2_ref, w2))):
            loads.append(pltpu.make_async_copy(src.at[j], dst.at[j], wsem.at[j, k]))
    for c in loads:
        c.start()

    @pl.when(first)
    def _():
        each(per * nb - 1, lambda i: x_copy(i + 1).start())

    barrier = pltpu.get_barrier_semaphore()
    for dz in range(ndp):
        for ds in range(npp):
            if dz or ds:
                pl.semaphore_signal(barrier, inc=1, device_id=((z + dz) % ndp, (s + ds) % npp), device_id_type=MESH)
    pl.semaphore_wait(barrier, ndp * npp - 1)

    def share_h(i):
        return pltpu.make_async_remote_copy(src_ref=hin.at[0, *part(i)], dst_ref=hin.at[1, *part(i)], send_sem=zhsend.at[i],
                                            recv_sem=xhrecv.at[i], device_id=peer, device_id_type=MESH)

    def share_g(m):
        return pltpu.make_async_remote_copy(src_ref=gin.at[0, m], dst_ref=gin.at[1, m], send_sem=zgsend.at[m],
                                            recv_sem=xgrecv.at[m], device_id=peer, device_id_type=MESH)

    def pass_h(i, k):
        return pltpu.make_async_remote_copy(src_ref=hst.at[k], dst_ref=hin.at[0, *part(i)], send_sem=hsend.at[k],
                                            recv_sem=hrecv.at[i], device_id=(z, lax.rem(s + 1, npp)), device_id_type=MESH)

    def pass_g(m, k):
        return pltpu.make_async_remote_copy(src_ref=gst.at[k], dst_ref=gin.at[0, m], send_sem=gsend.at[k], recv_sem=grecv.at[m],
                                            device_id=(z, lax.rem(s + npp - 1, npp)), device_id_type=MESH)

    def f_out(j, r, m):
        return (pltpu.make_async_copy(us.at[j], e_out.at[j, r, m], ussem.at[j, 0]),
                pltpu.make_async_copy(as_.at[j], a_out.at[j, r, m], assem.at[j, 0]))

    def f_out_part(j, i, k):
        m, rows = part(i)
        mine = pl.ds(pl.multiple_of(k * TF, TF), TF)
        return (pltpu.make_async_copy(us.at[j, mine], e_out.at[j, z, m, rows], ussem.at[j, k]),
                pltpu.make_async_copy(as_.at[j, mine], a_out.at[j, z, m, rows], assem.at[j, k]))

    def u_in(j, r, m):
        return pltpu.make_async_copy(e_out.at[j, r, m], ub.at[j], ubsem.at[j])

    def e_outc(j, r, m):
        return pltpu.make_async_copy(es.at[j], e_out.at[j, r, m], essem.at[j])

    def keep(src, dst, sem):
        return pltpu.make_async_copy(src, dst, sem)

    def gelu(j, rows):
        def point(q, c):
            cs = pl.ds(c * CH, CH)
            u = q.astype(BF)
            us[j, rows, cs] = u
            u = u.astype(F32)
            a = ((0.5 * u) * (1.0 + jnp.tanh(u * (C0 + C1 * (u * u))))).astype(BF)
            as_[j, rows, cs] = a
            return a
        return point

    def dgelu(j):
        def point(q, c):
            cs = pl.ds(c * CH, CH)
            u = jnp.clip(ub[j, :, cs], -30.0, 30.0).astype(F32)
            k = C1 * (u * u)
            th = jnp.tanh(u * (C0 + k))
            d = (1.0 + th) * (0.5 + (1.0 - th) * (u * (0.5 * C0 + 1.5 * k)))
            e = (d * q).astype(BF)
            es[j, :, cs] = e
            return e
        return point

    def fwd(j, x, rows, full=True):
        second = (lambda a, c: _nn(a, w2[j, pl.ds(c * CH, CH), :])) if full else None
        return _layer(x, nc, lambda x, c: _nn(x, w1[j, :, pl.ds(c * CH, CH)]), gelu(j, rows), second)

    def bwd(j, g, full=True):
        second = (lambda e, c: _nt(e, w1[j, :, pl.ds(c * CH, CH)])) if full else None
        return _layer(g, nc, lambda g, c: _nt(g, w2[j, pl.ds(c * CH, CH), :]), dgelu(j), second)

    def start(copies):
        for c in copies:
            c.start()

    def wait(copies):
        for c in copies:
            c.wait()

    def fwd_own(i):
        m, rows = part(i)
        k = lax.rem(i, 2)
        mine = pl.ds(pl.multiple_of(k * TF, TF), TF)
        x_copy(i).wait()
        share_h(i).start()
        keep(hin.at[0, m, rows], h_out.at[0, z, m, rows], hcp).start()

        @pl.when(i == 0)
        def _():
            wait(loads[:2])

        def h1_out():
            return keep(h1s.at[mine], h_out.at[1, z, m, rows], h1sem.at[k])

        @pl.when(i > 1)
        def _():
            wait(f_out_part(0, i, k))
            h1_out().wait()
        h1s[mine] = fwd(0, hin[0, m, rows], mine)
        start(f_out_part(0, i, k))
        h1_out().start()

        @pl.when(i == 0)
        def _():
            wait(loads[2:])

        @pl.when(i > 1)
        def _():
            wait(f_out_part(1, i, k))

            @pl.when(jnp.logical_not(last))
            def _():
                pass_h(i, k).wait_send()
        hst[k] = fwd(1, h1s[mine], mine)
        start(f_out_part(1, i, k))

        @pl.when(jnp.logical_not(last))
        def _():
            pass_h(i, k).start()

        @pl.when(last)
        def _():
            @pl.when(lax.rem(i, per) == 0)
            def _():
                t_copy(m).wait()
            d = hst[k].astype(F32) - gin[0, m, rows].astype(F32)
            gin[0, m, rows] = (d * inv).astype(BF)
            p = jnp.sum((d * d).reshape(TF // 8, 8, d.shape[-1]), axis=0)
            acc[...] += sum(p[:, c:c + 128] for c in range(0, d.shape[-1], 128))

    def fwd_other(m):
        r = 1 - z
        rows = pl.ds(0, T)
        for p in range(per):
            share_h(per * m + p).wait_recv()
        keep(hin.at[1, m], h_out.at[0, r, m], hcp).start()

        @pl.when(m > 0)
        def _():
            wait(f_out(0, r, m))
            keep(h1s, h_out.at[1, r, m], h1sem.at[0]).wait()
        h1s[...] = fwd(0, hin[1, m], rows)
        start(f_out(0, r, m))
        keep(h1s, h_out.at[1, r, m], h1sem.at[0]).start()

        @pl.when(m > 0)
        def _():
            wait(f_out(1, r, m))
        fwd(1, h1s[...], rows, full=False)
        start(f_out(1, r, m))

    def bwd_task(o, m, b):
        r = z if o == 0 else 1 - z
        if o == 0:
            @pl.when(jnp.logical_not(last))
            def _():
                t_copy(m).wait()
            share_g(m).start()
        else:
            share_g(m).wait_recv()
        keep(gin.at[o, m], g_out.at[1, r, m], gcp).start()

        def ready(j):
            @pl.when(b > 0)
            def _():
                e_outc(j, 0, 0).wait()
                if j == 1:
                    keep(g0s, g_out.at[0, r, m], g0sem).wait()
            u_in(j, r, m).wait()

        def ahead(j):
            @pl.when(m + 1 < nb)
            def _():
                u_in(j, r, m + 1).start()

        ready(1)
        g0s[...] = bwd(1, gin[o, m])
        e_outc(1, r, m).start()
        keep(g0s, g_out.at[0, r, m], g0sem).start()
        ahead(1)
        ready(0)
        if o == 0:
            k = m % 2

            @pl.when(jnp.logical_and(m > 1, jnp.logical_not(first)))
            def _():
                pass_g(m, k).wait_send()
            gst[k] = bwd(0, g0s[...])
        else:
            bwd(0, g0s[...], full=False)
        e_outc(0, r, m).start()
        ahead(0)
        if o == 0:
            @pl.when(jnp.logical_not(first))
            def _():
                pass_g(m, k).start()

    def loss_copy(dz, ds):
        return pltpu.make_async_remote_copy(src_ref=acc, dst_ref=loss_out.at[z], send_sem=lsend.at[dz * npp + ds],
                                            recv_sem=lrecv.at[z],
                                            device_id=((z + dz) % ndp, (s + ds) % npp), device_id_type=MESH)

    def loss_own():
        return pltpu.make_async_copy(acc, loss_out.at[z], lrecv.at[z])

    others = [(dz, ds) for dz in range(ndp) for ds in range(npp) if dz or ds]

    def send_loss():
        loss_own().start()
        for dz, ds in others:
            loss_copy(dz, ds).start()

    room = jnp.minimum(nb, (8 * (npp - 1 - s)) // 3)

    nf = per * nb
    a, b, c, d = nf + room, nf + room + nb, nf + 2 * nb, nf + 3 * nb

    def load_u(r):
        for j in (1, 0):
            u_in(j, r, 0).start()

    def task(i, carry):
        @pl.when(i < nf)
        def _():
            fwd_own(i)

        @pl.when(i == nf - 1)
        def _():
            for j in range(2):
                for k in range(2):
                    wait(f_out_part(j, 0, k))
            for k in range(2):
                keep(h1s.at[pl.ds(k * TF, TF)], h_out.at[1, z, 0, pl.ds(k * TF, TF)], h1sem.at[k]).wait()
            load_u(z)
            pl.when(last)(send_loss)

        early = jnp.logical_and(i >= nf, i < a)
        late = jnp.logical_and(i >= b, i < c)

        @pl.when(jnp.logical_or(early, late))
        def _():
            fwd_other(jnp.where(early, i - nf, i - nf - nb))

        @pl.when(jnp.logical_and(i >= a, i < b))
        def _():
            bwd_task(0, i - a, i - a)

        @pl.when(i == c - 1)
        def _():
            for j in range(2):
                wait(f_out(j, 0, 0))
            load_u(1 - z)

        @pl.when(i >= c)
        def _():
            bwd_task(1, i - c, i - c + nb)
        return carry

    lax.fori_loop(0, d, task, 0)

    @pl.when(last)
    def _():
        for dz, ds in others:
            loss_copy(dz, ds).wait_send()
    for d in range(ndp):
        pltpu.make_async_copy(acc, loss_out.at[d], lrecv.at[d]).wait()
    each(nf, lambda i: share_h(i).wait_send())
    each(nb, lambda m: share_g(m).wait_send())
    for k in range(2):
        @pl.when(jnp.logical_not(last))
        def _():
            pass_h(0, k).wait_send()

        @pl.when(jnp.logical_not(first))
        def _():
            pass_g(0, k).wait_send()
    keep(hin, h_out.at[0], hcp).wait()
    keep(gin, g_out.at[1], gcp).wait()
    keep(h1s, h_out.at[1, 0, 0], h1sem.at[0]).wait()
    keep(g0s, g_out.at[0, 0, 0], g0sem).wait()
    for j in range(2):
        e_outc(j, 0, 0).wait()


def _stages(x, t, w1, w2, ndp, npp, inv):
    nb, _, d = x.shape
    ff = w1.shape[-1]
    nf = nb * T // TF
    dma = pltpu.SemaphoreType.DMA
    act = jax.ShapeDtypeStruct((2, ndp, nb, T, d), BF)
    wide = jax.ShapeDtypeStruct((2, ndp, nb, T, ff), BF)
    flops = 28 * nb * T * d * ff
    return pl.pallas_call(
        functools.partial(_stage_kernel, ndp, npp, nb, inv),
        out_shape=(act, act, wide, wide, jax.ShapeDtypeStruct((ndp, 8, 128), F32)),
        in_specs=[ANY] * 4,
        out_specs=(ANY,) * 5,
        scratch_shapes=[
            pltpu.VMEM((2, d, ff), BF), pltpu.VMEM((2, ff, d), BF),
            pltpu.VMEM((ndp, nb, T, d), BF), pltpu.VMEM((ndp, nb, T, d), BF),
            pltpu.VMEM((2, T, ff), BF), pltpu.VMEM((2, T, ff), BF), pltpu.VMEM((2, T, ff), BF), pltpu.VMEM((2, T, ff), BF),
            pltpu.VMEM((T, d), BF), pltpu.VMEM((T, d), BF), pltpu.VMEM((2, TF, d), BF), pltpu.VMEM((2, T, d), BF),
            pltpu.VMEM((8, 128), F32),
            dma((2, 2)), dma((nf,)), dma((nb,)), dma((nf,)), dma((nb,)), dma((nf,)), dma((nb,)), dma, dma, dma((2,)), dma,
            dma((2, 2)), dma((2, 2)), dma((2,)), dma((2,)), dma((2,)), dma((2,)), dma((ndp * npp,)), dma((ndp,)),
        ],
        compiler_params=pltpu.CompilerParams(collective_id=0, has_side_effects=True, vmem_limit_bytes=67_043_328),
        cost_estimate=pl.CostEstimate(flops=flops, bytes_accessed=16 * nb * T * ff, transcendentals=8 * nb * T * ff),
        name="stage",
    )(x, t, w1, w2)


def _half_kernel(z_ref, h_ref, e_ref, o_ref):
    p = _tn(h_ref[...], e_ref[...])
    k = pl.program_id(0)

    @pl.when(k == 0)
    def _():
        o_ref[...] = p

    @pl.when(k > 0)
    def _():
        o_ref[...] += p


def _half(h, e, z):
    _, n, d = h.shape
    ff = e.shape[-1]
    step = 2048
    return pl.pallas_call(
        _half_kernel,
        grid_spec=pltpu.PrefetchScalarGridSpec(
            num_scalar_prefetch=1,
            grid=(n // step,),
            in_specs=[pl.BlockSpec((None, step, d), lambda k, z: (0, k, 0)),
                      pl.BlockSpec((None, step, ff // 2), lambda k, z: (0, k, z[0]))],
            out_specs=pl.BlockSpec((d, ff // 2), lambda k, z: (0, 0)),
        ),
        out_shape=jax.ShapeDtypeStruct((d, ff // 2), F32),
        compiler_params=pltpu.CompilerParams(vmem_limit_bytes=62 * 1024 * 1024),
        cost_estimate=pl.CostEstimate(flops=n * d * ff, bytes_accessed=n * (2 * d + ff), transcendentals=0),
        name="half",
    )(z, h, e)


def _dw_kernel(h_ref, e_ref, a_ref, g_ref, s_ref, o1_ref, o2_ref, res, tile, o1, o2, sv, rsem, tsem, osem, ssem, vsem):
    z = lax.axis_index("dp")
    ff = e_ref.shape[-1]
    w = tile.shape[-1]
    per = ff // w
    steps = 3 * per
    cols = lambda t: pl.ds(pl.multiple_of(t * w, w), w)

    def resident(p):
        slot = p % 2
        src = h_ref.at[1] if p == 0 else g_ref.at[p - 1]
        return pltpu.make_async_copy(src, res.at[slot], rsem.at[slot])

    def stream_e(i):
        return pltpu.make_async_copy(e_ref.at[1, :, cols(i)], tile.at[lax.rem(i, 2)], tsem.at[lax.rem(i, 2)])

    def stream_a(i):
        j = lax.div(i, per) - 1
        return pltpu.make_async_copy(a_ref.at[j, :, cols(i - per * (j + 1))], tile.at[lax.rem(i, 2)], tsem.at[lax.rem(i, 2)])

    def put1(i):
        return pltpu.make_async_copy(o1.at[lax.rem(i, 2)], o1_ref.at[1, :, cols(i)], osem.at[lax.rem(i, 2)])

    def put2(i):
        j = lax.div(i, per) - 1
        return pltpu.make_async_copy(o2.at[lax.rem(i, 2)], o2_ref.at[j, cols(i - per * (j + 1)), :], osem.at[lax.rem(i, 2)])

    halves = [(pltpu.make_async_copy(s_ref.at[:, pl.ds(t * w, w)], sv.at[t], ssem.at[t]),
               pltpu.make_async_copy(sv.at[t], o1_ref.at[0, :, cols(z * (per // 2) + t)], vsem.at[t])) for t in range(per // 2)]

    resident(0).start()
    stream_e(0).start()

    def step(i, carry):
        @pl.when(i + 1 < per)
        def _():
            stream_e(i + 1).start()

        @pl.when(jnp.logical_and(i + 1 >= per, i + 1 < steps))
        def _():
            stream_a(i + 1).start()

        for p in range(3):
            @pl.when(i == per * p)
            def _():
                resident(p).wait()

            if p < 2:
                @pl.when(i == per * p + 1)
                def _():
                    resident(p + 1).start()
        for t, (get, put) in enumerate(halves):
            @pl.when(i == 2 + 2 * t)
            def _():
                get.start()

            @pl.when(i == 3 + 2 * t)
            def _():
                get.wait()
                put.start()
        k = lax.rem(i, 2)
        pltpu.make_async_copy(e_ref.at[1, :, pl.ds(0, w)], tile.at[k], tsem.at[k]).wait()

        @pl.when(i > 1)
        def _():
            pltpu.make_async_copy(o1.at[k], o1_ref.at[1, :, pl.ds(0, w)], osem.at[k]).wait()
        r = lax.rem(lax.div(i, per), 2)

        @pl.when(i < per)
        def _():
            o1[k] = _tn(res[r], tile[k])
            put1(i).start()

        @pl.when(i >= per)
        def _():
            o2[k] = _tn(tile[k], res[r])
            put2(i).start()
        return carry

    lax.fori_loop(0, steps, step, 0)
    for i in (steps - 2, steps - 1):
        put2(jnp.int32(i)).wait()
    for _, put in halves:
        put.wait()


def _dw(h, e, a, g, half):
    n, d = h.shape[1:]
    ff = e.shape[-1]
    w = 512
    dma = pltpu.SemaphoreType.DMA
    return pl.pallas_call(
        _dw_kernel,
        out_shape=(jax.ShapeDtypeStruct((2, d, ff), F32), jax.ShapeDtypeStruct((2, ff, d), F32)),
        in_specs=[ANY] * 5,
        out_specs=(ANY, ANY),
        scratch_shapes=[
            pltpu.VMEM((2, n, d), BF), pltpu.VMEM((2, n, w), BF), pltpu.VMEM((2, d, w), F32), pltpu.VMEM((2, w, d), F32),
            pltpu.VMEM((ff // w // 2, d, w), F32),
            dma((2,)), dma((2,)), dma((2,)), dma((ff // w // 2,)), dma((ff // w // 2,)),
        ],
        compiler_params=pltpu.CompilerParams(vmem_limit_bytes=62 * 1024 * 1024),
        cost_estimate=pl.CostEstimate(flops=6 * n * d * ff, bytes_accessed=6 * n * ff, transcendentals=0),
        name="dw",
    )(h, e, a, g, half)


def solution(mesh):
    ndp = mesh.shape["dp"]
    npp = mesh.shape["pp"]

    def body(x, t, w1, w2):
        nm, tok, d = x.shape
        ff = w1.shape[-1]
        inv = 1.0 / (nm * tok * ndp * d)
        nb = nm * tok // T
        h, g, a, e, loss = _stages(x.reshape(nb, T, d), t.reshape(nb, T, d), w1[0], w2[0], ndp, npp, inv)
        n = ndp * nb * T
        h, g, a, e = (v.reshape(2, n, v.shape[-1]) for v in (h, g, a, e))
        z = lax.axis_index("dp")
        half = _half(h, e, jnp.full((1,), z, jnp.int32))
        other = lax.ppermute(half, "dp", [(i, (i + 1) % ndp) for i in range(ndp)])
        dw1, dw2 = _dw(h, e, a, g, half)
        dw1 = lax.dynamic_update_slice(dw1, other[None], (0, 0, (1 - z) * (ff // 2)))
        return dw1[None], dw2[None], 0.5 * inv * jnp.sum(loss)

    return jax.shard_map(body, mesh=mesh,
                         in_specs=(P(None, 'dp', None), P(None, 'dp', None), P('pp'), P('pp')),
                         out_specs=(P('pp'), P('pp'), P()), check_vma=False)
```

```python
import functools
import math

import jax
import jax.numpy as jnp
from jax import lax
from jax.experimental import pallas as pl
from jax.experimental.pallas import tpu as pltpu
from jax.sharding import PartitionSpec as P

MESH = pl.DeviceIdType.MESH
BF, F32 = jnp.bfloat16, jnp.float32
ANY = pl.BlockSpec(memory_space=pl.ANY)
C0 = math.sqrt(2.0 / math.pi)
C1 = C0 * 0.044715
T = 256
TF = 128
CH = 768
CHF = 1024


def _nn(a, b):
    return jnp.dot(a, b, preferred_element_type=F32)


def _nt(a, b):
    return lax.dot_general(a, b, (((1,), (1,)), ((), ())), preferred_element_type=F32)


def _tn(a, b):
    return lax.dot_general(a, b, (((0,), (0,)), ((), ())), preferred_element_type=F32)


def _layer(x, n, first, point, second):
    r = x.astype(F32)
    q = first(x, 0)
    for c in range(n):
        ahead = first(x, c + 1) if c + 1 < n else None
        a = point(q, c)
        if second is not None:
            r = r + second(a, c)
        q = ahead
    return None if second is None else r.astype(BF)


def _stage_kernel(ndp, npp, nb, inv, x_ref, t_ref, w1_ref, w2_ref,
                  h_out, g_out, a_out, e_out, loss_out,
                  w1, w2, hin, gin, us, as_, ub, es, h1s, g0s, hst, gst, acc,
                  wsem, hrecv, grecv, xhrecv, xgrecv, zhsend, zgsend, hcp, gcp, h1sem, g0sem,
                  ussem, assem, ubsem, essem, hsend, gsend, lsend, lrecv):
    z = lax.axis_index("dp")
    s = lax.axis_index("pp")
    peer = (1 - z, s)
    ff = w1.shape[-1]
    nc = ff // CH
    first, last = s == 0, s == npp - 1

    per = T // TF

    def part(i):
        return lax.div(i, per), pl.ds(pl.multiple_of(lax.rem(i, per) * TF, TF), TF)

    def x_copy(i):
        return pltpu.make_async_copy(x_ref.at[part(i)], hin.at[0, *part(i)], hrecv.at[i])

    def t_copy(m):
        return pltpu.make_async_copy(t_ref.at[m], gin.at[0, m], grecv.at[m])

    def each(n, f):
        def step(i, c):
            f(i)
            return c
        lax.fori_loop(0, n, step, 0)

    @pl.when(first)
    def _():
        x_copy(0).start()

    @pl.when(last)
    def _():
        each(nb, lambda m: t_copy(m).start())
        acc[...] = jnp.zeros_like(acc)

    loads = []
    for j in range(2):
        for k, (src, dst) in enumerate(((w1_ref, w1), (w2_ref, w2))):
            loads.append(pltpu.make_async_copy(src.at[j], dst.at[j], wsem.at[j, k]))
    for c in loads:
        c.start()

    @pl.when(first)
    def _():
        each(per * nb - 1, lambda i: x_copy(i + 1).start())

    barrier = pltpu.get_barrier_semaphore()
    for dz in range(ndp):
        for ds in range(npp):
            if dz or ds:
                pl.semaphore_signal(barrier, inc=1, device_id=((z + dz) % ndp, (s + ds) % npp), device_id_type=MESH)
    pl.semaphore_wait(barrier, ndp * npp - 1)

    def share_h(i):
        return pltpu.make_async_remote_copy(src_ref=hin.at[0, *part(i)], dst_ref=hin.at[1, *part(i)], send_sem=zhsend.at[i],
                                            recv_sem=xhrecv.at[i], device_id=peer, device_id_type=MESH)

    def share_g(m):
        return pltpu.make_async_remote_copy(src_ref=gin.at[0, m], dst_ref=gin.at[1, m], send_sem=zgsend.at[m],
                                            recv_sem=xgrecv.at[m], device_id=peer, device_id_type=MESH)

    def pass_h(i, k):
        return pltpu.make_async_remote_copy(src_ref=hst.at[k], dst_ref=hin.at[0, *part(i)], send_sem=hsend.at[k],
                                            recv_sem=hrecv.at[i], device_id=(z, lax.rem(s + 1, npp)), device_id_type=MESH)

    def pass_g(m, k):
        return pltpu.make_async_remote_copy(src_ref=gst.at[k], dst_ref=gin.at[0, m], send_sem=gsend.at[k], recv_sem=grecv.at[m],
                                            device_id=(z, lax.rem(s + npp - 1, npp)), device_id_type=MESH)

    def f_out(j, r, m):
        return (pltpu.make_async_copy(us.at[j], e_out.at[j, r, m], ussem.at[j, 0]),
                pltpu.make_async_copy(as_.at[j], a_out.at[j, r, m], assem.at[j, 0]))

    def f_out_part(j, i, k):
        m, rows = part(i)
        mine = pl.ds(pl.multiple_of(k * TF, TF), TF)
        return (pltpu.make_async_copy(us.at[j, mine], e_out.at[j, z, m, rows], ussem.at[j, k]),
                pltpu.make_async_copy(as_.at[j, mine], a_out.at[j, z, m, rows], assem.at[j, k]))

    def u_in(j, r, m):
        return pltpu.make_async_copy(e_out.at[j, r, m], ub.at[j], ubsem.at[j])

    def e_outc(j, r, m):
        return pltpu.make_async_copy(es.at[j], e_out.at[j, r, m], essem.at[j])

    def keep(src, dst, sem):
        return pltpu.make_async_copy(src, dst, sem)

    def gelu(j, rows, ch):
        def point(q, c):
            cs = pl.ds(c * ch, ch)
            u = q.astype(BF)
            us[j, rows, cs] = u
            u = u.astype(F32)
            a = ((0.5 * u) * (1.0 + jnp.tanh(u * (C0 + C1 * (u * u))))).astype(BF)
            as_[j, rows, cs] = a
            return a
        return point

    def dgelu(j):
        def point(q, c):
            cs = pl.ds(c * CH, CH)
            u = jnp.clip(ub[j, :, cs], -30.0, 30.0).astype(F32)
            k = C1 * (u * u)
            th = jnp.tanh(u * (C0 + k))
            d = (1.0 + th) * (0.5 + (1.0 - th) * (u * (0.5 * C0 + 1.5 * k)))
            e = (d * q).astype(BF)
            es[j, :, cs] = e
            return e
        return point

    def fwd(j, x, rows, full=True):
        ch = CH if x.shape[0] == T else CHF
        second = (lambda a, c: _nn(a, w2[j, pl.ds(c * ch, ch), :])) if full else None
        return _layer(x, ff // ch, lambda x, c: _nn(x, w1[j, :, pl.ds(c * ch, ch)]), gelu(j, rows, ch), second)

    def bwd(j, g, full=True):
        second = (lambda e, c: _nt(e, w1[j, :, pl.ds(c * CH, CH)])) if full else None
        return _layer(g, nc, lambda g, c: _nt(g, w2[j, pl.ds(c * CH, CH), :]), dgelu(j), second)

    def start(copies):
        for c in copies:
            c.start()

    def wait(copies):
        for c in copies:
            c.wait()

    def fwd_own(i):
        m, rows = part(i)
        k = lax.rem(i, 2)
        mine = pl.ds(pl.multiple_of(k * TF, TF), TF)
        x_copy(i).wait()
        share_h(i).start()
        keep(hin.at[0, m, rows], h_out.at[0, z, m, rows], hcp).start()

        @pl.when(i == 0)
        def _():
            wait(loads[:2])

        def h1_out():
            return keep(h1s.at[mine], h_out.at[1, z, m, rows], h1sem.at[k])

        @pl.when(i > 1)
        def _():
            wait(f_out_part(0, i, k))
            h1_out().wait()
        h1s[mine] = fwd(0, hin[0, m, rows], mine)
        start(f_out_part(0, i, k))
        h1_out().start()

        @pl.when(i == 0)
        def _():
            wait(loads[2:])

        @pl.when(i > 1)
        def _():
            wait(f_out_part(1, i, k))

            @pl.when(jnp.logical_not(last))
            def _():
                pass_h(i, k).wait_send()
        hst[k] = fwd(1, h1s[mine], mine)

        @pl.when(jnp.logical_not(last))
        def _():
            pass_h(i, k).start()
        start(f_out_part(1, i, k))

        @pl.when(last)
        def _():
            @pl.when(lax.rem(i, per) == 0)
            def _():
                t_copy(m).wait()
            d = hst[k].astype(F32) - gin[0, m, rows].astype(F32)
            gin[0, m, rows] = (d * inv).astype(BF)
            p = jnp.sum((d * d).reshape(TF // 8, 8, d.shape[-1]), axis=0)
            acc[...] += sum(p[:, c:c + 128] for c in range(0, d.shape[-1], 128))

    def fwd_other(m):
        r = 1 - z
        rows = pl.ds(0, T)
        for p in range(per):
            share_h(per * m + p).wait_recv()
        keep(hin.at[1, m], h_out.at[0, r, m], hcp).start()

        @pl.when(m > 0)
        def _():
            wait(f_out(0, r, m))
            keep(h1s, h_out.at[1, r, m], h1sem.at[0]).wait()
        h1s[...] = fwd(0, hin[1, m], rows)
        start(f_out(0, r, m))
        keep(h1s, h_out.at[1, r, m], h1sem.at[0]).start()

        @pl.when(m > 0)
        def _():
            wait(f_out(1, r, m))
        fwd(1, h1s[...], rows, full=False)
        start(f_out(1, r, m))

    def bwd_task(o, m, b):
        r = z if o == 0 else 1 - z
        if o == 0:
            @pl.when(jnp.logical_not(last))
            def _():
                t_copy(m).wait()
            share_g(m).start()
        else:
            share_g(m).wait_recv()
        keep(gin.at[o, m], g_out.at[1, r, m], gcp).start()

        def ready(j):
            @pl.when(b > 0)
            def _():
                e_outc(j, 0, 0).wait()
                if j == 1:
                    keep(g0s, g_out.at[0, r, m], g0sem).wait()
            u_in(j, r, m).wait()

        def ahead(j):
            @pl.when(m + 1 < nb)
            def _():
                u_in(j, r, m + 1).start()

        ready(1)
        g0s[...] = bwd(1, gin[o, m])
        e_outc(1, r, m).start()
        keep(g0s, g_out.at[0, r, m], g0sem).start()
        ahead(1)
        ready(0)
        if o == 0:
            k = m % 2

            @pl.when(jnp.logical_and(m > 1, jnp.logical_not(first)))
            def _():
                pass_g(m, k).wait_send()
            gst[k] = bwd(0, g0s[...])
        else:
            bwd(0, g0s[...], full=False)
        if o == 0:
            @pl.when(jnp.logical_not(first))
            def _():
                pass_g(m, k).start()
        e_outc(0, r, m).start()
        ahead(0)

    def loss_copy(dz, ds):
        return pltpu.make_async_remote_copy(src_ref=acc, dst_ref=loss_out.at[z], send_sem=lsend.at[dz * npp + ds],
                                            recv_sem=lrecv.at[z],
                                            device_id=((z + dz) % ndp, (s + ds) % npp), device_id_type=MESH)

    def loss_own():
        return pltpu.make_async_copy(acc, loss_out.at[z], lrecv.at[z])

    others = [(dz, ds) for dz in range(ndp) for ds in range(npp) if dz or ds]

    def send_loss():
        loss_own().start()
        for dz, ds in others:
            loss_copy(dz, ds).start()

    room = jnp.minimum(nb, (37 * (npp - 1 - s) + 1) // 10)

    nf = per * nb
    a, b, c, d = nf + room, nf + room + nb, nf + 2 * nb, nf + 3 * nb

    def load_u(r):
        for j in (1, 0):
            u_in(j, r, 0).start()

    def task(i, carry):
        @pl.when(i < nf)
        def _():
            fwd_own(i)

        @pl.when(i == nf - 1)
        def _():
            for j in range(2):
                for k in range(2):
                    wait(f_out_part(j, 0, k))
            for k in range(2):
                keep(h1s.at[pl.ds(k * TF, TF)], h_out.at[1, z, 0, pl.ds(k * TF, TF)], h1sem.at[k]).wait()
            load_u(z)
            pl.when(last)(send_loss)

        early = jnp.logical_and(i >= nf, i < a)
        late = jnp.logical_and(i >= b, i < c)

        @pl.when(jnp.logical_or(early, late))
        def _():
            fwd_other(jnp.where(early, i - nf, i - nf - nb))

        @pl.when(jnp.logical_and(i >= a, i < b))
        def _():
            bwd_task(0, i - a, i - a)

        @pl.when(i == c - 1)
        def _():
            for j in range(2):
                wait(f_out(j, 0, 0))
            load_u(1 - z)

        @pl.when(i >= c)
        def _():
            bwd_task(1, i - c, i - c + nb)
        return carry

    lax.fori_loop(0, d, task, 0)

    @pl.when(last)
    def _():
        for dz, ds in others:
            loss_copy(dz, ds).wait_send()
    for d in range(ndp):
        pltpu.make_async_copy(acc, loss_out.at[d], lrecv.at[d]).wait()
    each(nf, lambda i: share_h(i).wait_send())
    each(nb, lambda m: share_g(m).wait_send())
    for k in range(2):
        @pl.when(jnp.logical_not(last))
        def _():
            pass_h(0, k).wait_send()

        @pl.when(jnp.logical_not(first))
        def _():
            pass_g(0, k).wait_send()
    keep(hin, h_out.at[0], hcp).wait()
    keep(gin, g_out.at[1], gcp).wait()
    keep(h1s, h_out.at[1, 0, 0], h1sem.at[0]).wait()
    keep(g0s, g_out.at[0, 0, 0], g0sem).wait()
    for j in range(2):
        e_outc(j, 0, 0).wait()


def _stages(x, t, w1, w2, ndp, npp, inv):
    nb, _, d = x.shape
    ff = w1.shape[-1]
    nf = nb * T // TF
    dma = pltpu.SemaphoreType.DMA
    act = jax.ShapeDtypeStruct((2, ndp, nb, T, d), BF)
    wide = jax.ShapeDtypeStruct((2, ndp, nb, T, ff), BF)
    flops = 28 * nb * T * d * ff
    return pl.pallas_call(
        functools.partial(_stage_kernel, ndp, npp, nb, inv),
        out_shape=(act, act, wide, wide, jax.ShapeDtypeStruct((ndp, 8, 128), F32)),
        in_specs=[ANY] * 4,
        out_specs=(ANY,) * 5,
        scratch_shapes=[
            pltpu.VMEM((2, d, ff), BF), pltpu.VMEM((2, ff, d), BF),
            pltpu.VMEM((ndp, nb, T, d), BF), pltpu.VMEM((ndp, nb, T, d), BF),
            pltpu.VMEM((2, T, ff), BF), pltpu.VMEM((2, T, ff), BF), pltpu.VMEM((2, T, ff), BF), pltpu.VMEM((2, T, ff), BF),
            pltpu.VMEM((T, d), BF), pltpu.VMEM((T, d), BF), pltpu.VMEM((2, TF, d), BF), pltpu.VMEM((2, T, d), BF),
            pltpu.VMEM((8, 128), F32),
            dma((2, 2)), dma((nf,)), dma((nb,)), dma((nf,)), dma((nb,)), dma((nf,)), dma((nb,)), dma, dma, dma((2,)), dma,
            dma((2, 2)), dma((2, 2)), dma((2,)), dma((2,)), dma((2,)), dma((2,)), dma((ndp * npp,)), dma((ndp,)),
        ],
        compiler_params=pltpu.CompilerParams(collective_id=0, has_side_effects=True, vmem_limit_bytes=67_043_328),
        cost_estimate=pl.CostEstimate(flops=flops, bytes_accessed=16 * nb * T * ff, transcendentals=8 * nb * T * ff),
        name="stage",
    )(x, t, w1, w2)


def _half_kernel(z_ref, h_ref, e_ref, o_ref):
    @pl.when(pl.program_id(0) == 0)
    def _():
        o_ref[...] = jnp.zeros_like(o_ref)
    for c in range(0, o_ref.shape[-1], 512):
        o_ref[:, c:c + 512] += _tn(h_ref[...], e_ref[:, c:c + 512])


def _half(h, e, z):
    _, n, d = h.shape
    ff = e.shape[-1]
    step = 2048
    return pl.pallas_call(
        _half_kernel,
        grid_spec=pltpu.PrefetchScalarGridSpec(
            num_scalar_prefetch=1,
            grid=(n // step,),
            in_specs=[pl.BlockSpec((None, step, d), lambda k, z: (0, k, 0)),
                      pl.BlockSpec((None, step, ff // 2), lambda k, z: (0, k, z[0]))],
            out_specs=pl.BlockSpec((d, ff // 2), lambda k, z: (0, 0)),
        ),
        out_shape=jax.ShapeDtypeStruct((d, ff // 2), F32),
        compiler_params=pltpu.CompilerParams(vmem_limit_bytes=62 * 1024 * 1024),
        cost_estimate=pl.CostEstimate(flops=n * d * ff, bytes_accessed=n * (2 * d + ff), transcendentals=0),
        name="half",
    )(z, h, e)


def _dw_kernel(h_ref, e_ref, a_ref, g_ref, s_ref, o1_ref, o2_ref, res, tile, o1, o2, sv, rsem, tsem, osem, ssem, vsem):
    z = lax.axis_index("dp")
    ff = e_ref.shape[-1]
    w = tile.shape[-1]
    per = ff // w
    steps = 3 * per
    cols = lambda t: pl.ds(pl.multiple_of(t * w, w), w)

    def resident(p):
        slot = p % 2
        src = h_ref.at[1] if p == 0 else g_ref.at[p - 1]
        return pltpu.make_async_copy(src, res.at[slot], rsem.at[slot])

    def stream_e(i):
        return pltpu.make_async_copy(e_ref.at[1, :, cols(i)], tile.at[lax.rem(i, 2)], tsem.at[lax.rem(i, 2)])

    def stream_a(i):
        j = lax.div(i, per) - 1
        return pltpu.make_async_copy(a_ref.at[j, :, cols(i - per * (j + 1))], tile.at[lax.rem(i, 2)], tsem.at[lax.rem(i, 2)])

    def put1(i):
        return pltpu.make_async_copy(o1.at[lax.rem(i, 2)], o1_ref.at[1, :, cols(i)], osem.at[lax.rem(i, 2)])

    def put2(i):
        j = lax.div(i, per) - 1
        return pltpu.make_async_copy(o2.at[lax.rem(i, 2)], o2_ref.at[j, cols(i - per * (j + 1)), :], osem.at[lax.rem(i, 2)])

    halves = [(pltpu.make_async_copy(s_ref.at[:, pl.ds(t * w, w)], sv.at[t], ssem.at[t]),
               pltpu.make_async_copy(sv.at[t], o1_ref.at[0, :, cols(z * (per // 2) + t)], vsem.at[t])) for t in range(per // 2)]

    resident(0).start()
    stream_e(0).start()

    def step(i, carry):
        @pl.when(i + 1 < per)
        def _():
            stream_e(i + 1).start()

        @pl.when(jnp.logical_and(i + 1 >= per, i + 1 < steps))
        def _():
            stream_a(i + 1).start()

        for p in range(3):
            @pl.when(i == per * p)
            def _():
                resident(p).wait()

            if p < 2:
                @pl.when(i == per * p + 1)
                def _():
                    resident(p + 1).start()
        for t, (get, put) in enumerate(halves):
            @pl.when(i == 2 + 2 * t)
            def _():
                get.start()

            @pl.when(i == 3 + 2 * t)
            def _():
                get.wait()
                put.start()
        k = lax.rem(i, 2)
        pltpu.make_async_copy(e_ref.at[1, :, pl.ds(0, w)], tile.at[k], tsem.at[k]).wait()

        @pl.when(i > 1)
        def _():
            pltpu.make_async_copy(o1.at[k], o1_ref.at[1, :, pl.ds(0, w)], osem.at[k]).wait()
        r = lax.rem(lax.div(i, per), 2)

        @pl.when(i < per)
        def _():
            o1[k] = _tn(res[r], tile[k])
            put1(i).start()

        @pl.when(i >= per)
        def _():
            o2[k] = _tn(tile[k], res[r])
            put2(i).start()
        return carry

    lax.fori_loop(0, steps, step, 0)
    for i in (steps - 2, steps - 1):
        put2(jnp.int32(i)).wait()
    for _, put in halves:
        put.wait()


def _dw(h, e, a, g, half):
    n, d = h.shape[1:]
    ff = e.shape[-1]
    w = 512
    dma = pltpu.SemaphoreType.DMA
    return pl.pallas_call(
        _dw_kernel,
        out_shape=(jax.ShapeDtypeStruct((2, d, ff), F32), jax.ShapeDtypeStruct((2, ff, d), F32)),
        in_specs=[ANY] * 5,
        out_specs=(ANY, ANY),
        scratch_shapes=[
            pltpu.VMEM((2, n, d), BF), pltpu.VMEM((2, n, w), BF), pltpu.VMEM((2, d, w), F32), pltpu.VMEM((2, w, d), F32),
            pltpu.VMEM((ff // w // 2, d, w), F32),
            dma((2,)), dma((2,)), dma((2,)), dma((ff // w // 2,)), dma((ff // w // 2,)),
        ],
        compiler_params=pltpu.CompilerParams(vmem_limit_bytes=62 * 1024 * 1024),
        cost_estimate=pl.CostEstimate(flops=6 * n * d * ff, bytes_accessed=6 * n * ff, transcendentals=0),
        name="dw",
    )(h, e, a, g, half)


def solution(mesh):
    ndp = mesh.shape["dp"]
    npp = mesh.shape["pp"]

    def body(x, t, w1, w2):
        nm, tok, d = x.shape
        ff = w1.shape[-1]
        inv = 1.0 / (nm * tok * ndp * d)
        nb = nm * tok // T
        h, g, a, e, loss = _stages(x.reshape(nb, T, d), t.reshape(nb, T, d), w1[0], w2[0], ndp, npp, inv)
        n = ndp * nb * T
        h, g, a, e = (v.reshape(2, n, v.shape[-1]) for v in (h, g, a, e))
        z = lax.axis_index("dp")
        half = _half(h, e, jnp.full((1,), z, jnp.int32))
        other = lax.ppermute(half, "dp", [(i, (i + 1) % ndp) for i in range(ndp)])
        dw1, dw2 = _dw(h, e, a, g, half)
        dw1 = lax.dynamic_update_slice(dw1, other[None], (0, 0, (1 - z) * (ff // 2)))
        return dw1[None], dw2[None], 0.5 * inv * jnp.sum(loss)

    return jax.shard_map(body, mesh=mesh,
                         in_specs=(P(None, 'dp', None), P(None, 'dp', None), P('pp'), P('pp')),
                         out_specs=(P('pp'), P('pp'), P()), check_vma=False)
```
